32 devices in a mesh: tensor: 4 (over y, x), expert: 4 (over z), dp: 2 (over core).
Axes of the slice: x: 2, y: 2, z: 4, core: 2. Of those that a mesh axis runs over, the one named last changes fastest.
Arguments:
- tokens: bfloat16 [1024, 2048], P(('dp', 'expert'), 'tensor'), parts along dimension 0, may hold values from -6 to 6
- expert_ids: int32 [1024, 8], P(('dp', 'expert')), parts along dimension 0, may hold values from 0 to 15, as said below
- combine_weight: bfloat16 [1024, 8], P(('dp', 'expert')), parts along dimension 0, may hold values from 0.049804688 to 1
- gate_weight: bfloat16 [16, 768, 2048], P('expert', 'tensor'), may hold values from -0.125 to 0.125
- up_weight: bfloat16 [16, 768, 2048], P('expert', 'tensor'), may hold values from -0.125 to 0.125
- down_weight: bfloat16 [16, 768, 2048], P('expert', 'tensor'), may hold values from -0.21875 to 0.21875
Outputs:
- mixed: bfloat16 [1024, 2048], P(('dp', 'expert'), 'tensor'), parts along dimension 0
The draws below stay inside these ranges and needn't reach their ends.
There are 2 independent parts, one for each index of `dp`. The reference program is written for one: setup_inputs(seed, part) draws one part's arguments, and reference() takes and returns one part's arrays. A program takes and returns all parts, laid end to end along the dimension named above; an argument that names none is the same for every part. Nothing has to cross between parts.
Inputs may be any that keep to these rules, and one draw needn't show every extreme that they name: `expert_ids`: each row names 8 different experts; expert e sits on index e // 4 of expert. The experts of one row sit on exactly 2 different indices, at most 4 on one index. Among the rows of one index of expert (aligned blocks of 128 rows), at most 96 rows name experts on any one index, and in every draw some index receives exactly 96 rows from every block. Over all blocks at most 384 rows name any one expert, and in every draw some expert is named by exactly 384 rows.
All inputs are finite; a program needn't handle non-finite values.
Results may differ from the reference program's by a relative error of at most 0.0098.
Values may be sent and summed in bfloat16 or wider, within the bound.
No kernel may reach another device: no remote copies, remote signals or barrier semaphores. Data moves between devices by JAX's collectives and lax.ppermute only.
A program may use at most 128 MiB of HBM per device.

```python
import math
import jax
import jax.numpy as jnp
from jax import lax

D = 2048
FF = 768
TOP = 8
EXP_DEV = 4
TOK_DEV = 128
EXPERTS = 16
TOKENS = 512


def draw_routing(key):
    device_count = EXPERTS // EXP_DEV
    block_count = TOKENS // TOK_DEV
    spread = min(6, device_count // 2)
    capacity = min(TOK_DEV * 3 // 4, 2 * TOK_DEV * spread // device_count)
    base_share = TOP // spread
    extra_share = TOP % spread
    most_share = base_share + (1 if extra_share > 0 else 0)
    key_bias, key_noise, key_favored, key_local = jax.random.split(jax.random.fold_in(key, 913), 4)
    favored = jax.random.randint(key_favored, (), 0, device_count)
    device_index = jnp.arange(device_count, dtype=jnp.int32)
    bias = jax.random.randint(key_bias, (device_count,), 0, 48)
    bias = jnp.where(device_index == favored, 100000, bias)
    noise = jax.random.randint(key_noise, (block_count, TOK_DEV, device_count), 0, 64)
    scores = ((noise + bias[None, None, :]) * 1024 + device_index[None, None, :]).astype(jnp.int32)
    block_start = jax.random.randint(key_local, (block_count, device_count), 0, EXP_DEV).astype(jnp.int32)
    shares = jnp.array([base_share + (1 if position < extra_share else 0) for position in range(spread)], jnp.int32)
    step_index = jnp.arange(most_share, dtype=jnp.int32)

    def route_block(block_scores, start_row):

        def take_row(carry, row_scores):
            counts, used = carry
            live_scores = jnp.where(counts < capacity, row_scores, -1)
            top_values, picked = lax.top_k(live_scores, spread)
            picked = picked.astype(jnp.int32)
            cursor = used[picked] + start_row[picked]
            local = ((cursor[:, None] + step_index[None, :]) % EXP_DEV).astype(jnp.int32)
            chosen = jnp.zeros((device_count,), jnp.int32).at[picked].set(1)
            used_next = used.at[picked].add(shares)
            return ((counts + chosen, used_next), (picked, local))
        zeros = jnp.zeros((device_count,), jnp.int32)
        _, outputs = lax.scan(take_row, (zeros, zeros), block_scores)
        return outputs
    picked, local = jax.vmap(route_block)(scores, block_start)
    columns = []
    for position in range(spread):
        share = base_share + (1 if position < extra_share else 0)
        columns.append(picked[:, :, position, None] * EXP_DEV + local[:, :, position, :share])
    chosen_ids = jnp.concatenate(columns, axis=-1)
    return chosen_ids.reshape(TOKENS, TOP).astype(jnp.int32)


def draw_expert_ids(key, part):
    return draw_routing(key)


def steps_of(key, extent, pieces, smallest, high):
    factor_of = 1.0
    for dim, shards_of in pieces:
        draws = jax.random.uniform(jax.random.fold_in(jax.random.fold_in(key, 6), dim), (shards_of,), jnp.float32, smallest / len(pieces), high / len(pieces))
        factor_of = factor_of * jnp.repeat(jnp.exp(draws), extent[dim] // shards_of).reshape((-1,) + (1,) * (len(extent) - 1 - dim))
    return factor_of


def bell_draw(key, dims, scale, most, pieces=(), held_as=jnp.bfloat16):
    values = jax.random.normal(key, dims, jnp.float32) * scale
    if len(pieces) > 0:
        values = steps_of(key, dims, pieces, -0.22, 0.18) * values
    return jnp.clip(values, min=-most, max=most).astype(held_as)


def setup_inputs(seed: int = 0, part: int = 0) -> dict:
    arg_keys = jax.random.split(jax.random.key(seed), 7)
    part_keys = jax.random.split(jax.random.fold_in(arg_keys[6], part), 7)
    tokens = bell_draw(part_keys[0], (TOKENS, D), 1.0, 6.0, ((0, 4), (1, 4)))
    expert_ids = draw_expert_ids(jax.random.fold_in(jax.random.fold_in(arg_keys[6], part), 71), part)
    combine_weight = jnp.clip(jnp.exp(math.log(1.0) - 2.9996462 * jax.random.uniform(part_keys[2], (TOKENS, TOP), jnp.float32) ** steps_of(part_keys[2], (TOKENS, TOP), ((0, 4),), -0.2, 0.2)), 0.049804688, 1.0).astype(jnp.bfloat16)
    gate_weight = bell_draw(arg_keys[3], (EXPERTS, FF, D), D ** -0.5, 0.125, ((0, 4), (1, 4)))
    up_weight = bell_draw(arg_keys[4], (EXPERTS, FF, D), D ** -0.5, 0.125, ((0, 4), (1, 4)))
    down_weight = bell_draw(arg_keys[5], (EXPERTS, FF, D), FF ** -0.5, 0.21875, ((0, 4), (1, 4)))
    return {"tokens": tokens, "expert_ids": expert_ids, "combine_weight": combine_weight, "gate_weight": gate_weight, "up_weight": up_weight, "down_weight": down_weight}


tile_rows = 128


def project_rows(inputs, weight_rows):
    return lax.dot_general(inputs, weight_rows, (((1,), (1,)), ((), ())), preferred_element_type=jnp.float32)


def reference(tokens, expert_ids, combine_weight, gate_weight, up_weight, down_weight):
    token_count = tokens.shape[0]
    expert_count = gate_weight.shape[0]
    top_count = expert_ids.shape[1]
    pair_count = token_count * top_count
    flat_expert = expert_ids.reshape(-1).astype(jnp.int32)
    flat_token = (jnp.arange(pair_count, dtype=jnp.int32) // top_count).astype(jnp.int32)
    flat_weight = combine_weight.reshape(-1).astype(jnp.float32)
    counts = jnp.zeros((expert_count,), jnp.int32).at[flat_expert].add(1)
    padded = ((counts + tile_rows - 1) // tile_rows * tile_rows).astype(jnp.int32)
    starts = (jnp.cumsum(padded) - padded).astype(jnp.int32)
    plain_start = (jnp.cumsum(counts) - counts).astype(jnp.int32)
    ordering = jnp.argsort(flat_expert, stable=True).astype(jnp.int32)
    sorted_expert = flat_expert[ordering]
    placement = (starts[sorted_expert] + jnp.arange(pair_count, dtype=jnp.int32) - plain_start[sorted_expert]).astype(jnp.int32)
    tile_count = pair_count // tile_rows + expert_count + 1
    slot_token = jnp.zeros((tile_count * tile_rows,), jnp.int32).at[placement].set(flat_token[ordering])
    slot_weight = jnp.zeros((tile_count * tile_rows,), jnp.float32).at[placement].set(flat_weight[ordering])
    tile_start = (jnp.arange(tile_count, dtype=jnp.int32) * tile_rows).astype(jnp.int32)
    tile_expert = jnp.clip(jnp.sum((starts[None, :] <= tile_start[:, None]).astype(jnp.int32), axis=1) - 1, 0, expert_count - 1).astype(jnp.int32)

    def visit_tile(accumulated, tile_index):
        row_tokens = lax.dynamic_slice_in_dim(slot_token, tile_index * tile_rows, tile_rows)
        row_weights = lax.dynamic_slice_in_dim(slot_weight, tile_index * tile_rows, tile_rows)
        tile_owner = tile_expert[tile_index]
        inputs = tokens[row_tokens]
        gate_value = project_rows(inputs, gate_weight[tile_owner])
        up_value = project_rows(inputs, up_weight[tile_owner])
        hidden = (jax.nn.silu(gate_value) * up_value).astype(jnp.bfloat16)
        expert_out = jnp.dot(hidden, down_weight[tile_owner], preferred_element_type=jnp.float32)
        return accumulated.at[row_tokens].add(row_weights[:, None] * expert_out), None

    accumulated, _ = lax.scan(visit_tile, jnp.zeros((token_count, tokens.shape[1]), jnp.float32), jnp.arange(tile_count, dtype=jnp.int32))
    return accumulated.astype(jnp.bfloat16)
```

```python
import functools

import jax
import jax.numpy as jnp
from jax import lax
from jax.experimental import pallas as pl
from jax.experimental.pallas import tpu as pltpu
from jax.sharding import PartitionSpec as P

MARK = 4096.0
VMEM = pltpu.VMEM
MIB = 1024 * 1024


def nt_dot(left, right):
    return lax.dot_general(left, right, (((1,), (1,)), ((), ())), preferred_element_type=jnp.float32)


def tn_dot(left, right):
    return lax.dot_general(left, right, (((0,), (0,)), ((), ())), preferred_element_type=jnp.float32)


def nn_dot(left, right):
    return jnp.dot(left, right, preferred_element_type=jnp.float32)


def iota(shape, dim):
    return lax.broadcasted_iota(jnp.int32, shape, dim)


def lanes(count):
    return -(-count // 128) * 128


def peer(index, step, count):
    if count & (count - 1) == 0:
        return index ^ step
    return (index + step) % count


def back(index, step, count):
    if count & (count - 1) == 0:
        return index ^ step
    return (index - step) % count


def exchange(value, axis, step, count):
    return lax.ppermute(value, axis, [(i, peer(i, step, count)) for i in range(count)])


def give_back(value, axis, step, count):
    return lax.ppermute(value, axis, [(i, back(i, step, count)) for i in range(count)])


def select_kernel(dest_count, capacity, local_count, dests, ids_ref, weight_ref, tokens_ref, *refs):
    row_refs, share_refs, placed_ref, slot_ref = refs[:dest_count], refs[dest_count:-2], refs[-2], refs[-1]
    tok_count, top_count = ids_ref.shape
    ids = ids_ref[...]
    weights = weight_ref[...].astype(jnp.float32)
    dest_lane = iota((tok_count, lanes(dest_count)), 1) * local_count
    expert_lane = iota((tok_count, lanes(dest_count * local_count)), 1)
    present = jnp.zeros(dest_lane.shape, jnp.float32)
    dense = jnp.zeros(expert_lane.shape, jnp.float32)
    for choice in range(top_count):
        chosen = ids[:, choice : choice + 1]
        present = jnp.where((chosen >= dest_lane) & (chosen < dest_lane + local_count), 1.0, present)
        dense = jnp.where(chosen == expert_lane, weights[:, choice : choice + 1], dense)
    dense = dense.astype(jnp.bfloat16)
    first, second = iota((tok_count, tok_count), 0), iota((tok_count, tok_count), 1)
    order = jnp.where(first < second, 1.0, jnp.where(first == second, MARK, 0.0)).astype(jnp.bfloat16)
    slot_ref[...] = tn_dot(present.astype(jnp.bfloat16), order)
    tokens = tokens_ref[...]
    wide = lanes(capacity)
    for step in range(dest_count):
        dest = dests(step)
        slots = iota((wide, tok_count), 0).astype(jnp.float32) + MARK
        placed = (slot_ref[pl.ds(dest, 1), :] == slots).astype(jnp.float32).astype(jnp.bfloat16)
        row_refs[step][...] = nn_dot(placed[:capacity], tokens).astype(jnp.bfloat16).reshape(row_refs[step].shape)
        pick_shape = (8, dense.shape[1])
        pick = (iota(pick_shape, 1) == dest * local_count + iota(pick_shape, 0)) & (iota(pick_shape, 0) < local_count)
        mine = nt_dot(pick.astype(jnp.float32).astype(jnp.bfloat16), dense).astype(jnp.bfloat16)
        share_refs[step][...] = nt_dot(mine, placed).astype(jnp.bfloat16).reshape(share_refs[step].shape)
        placed_ref[pl.ds(step * capacity, capacity), :] = placed[:capacity]


def expert_kernel(tensor_count, features, hidden_part, *refs):
    row_refs, (share_ref, gate_ref, up_ref, down_ref) = refs[:tensor_count], refs[tensor_count : tensor_count + 4]
    out_refs, rows_ref = refs[tensor_count + 4 : -1], refs[-1]
    capacity, width = row_refs[0].shape[-2:]
    for step in range(tensor_count):
        rows_ref[:, pl.ds(pl.multiple_of(features(step) * width, 128), width)] = row_refs[step][...].reshape(
            capacity, width
        )
    rows = rows_ref[...]
    gate_value = nt_dot(rows, gate_ref[...])
    up_value = nt_dot(rows, up_ref[...])
    hidden_count = gate_ref.shape[0]
    share = share_ref[...].reshape(share_ref.shape[-2:])
    slot_lanes = share.shape[1]
    eye = (iota((capacity, slot_lanes), 0) == iota((capacity, slot_lanes), 1)).astype(jnp.float32)
    by_slot = nt_dot(eye.astype(jnp.bfloat16), share).astype(jnp.bfloat16)
    spread_shape = (share.shape[0], hidden_count)
    start = iota(spread_shape, 0) * hidden_part
    spread = (iota(spread_shape, 1) >= start) & (iota(spread_shape, 1) < start + hidden_part)
    weight = nn_dot(by_slot, spread.astype(jnp.float32).astype(jnp.bfloat16))
    hidden = (gate_value / (1.0 + jnp.exp(-gate_value)) * up_value * weight).astype(jnp.bfloat16)
    for step in range(tensor_count):
        target = pl.ds(pl.multiple_of(features(step) * width, 128), width)
        part = nn_dot(hidden, down_ref[:, target])
        out_refs[step][...] = part.astype(out_refs[step].dtype).reshape(out_refs[step].shape)


def combine_kernel(placed_ref, *refs):
    row_refs, out_ref, all_ref = refs[:-2], refs[-2], refs[-1]
    start = 0
    for row_ref in row_refs:
        count = row_ref.shape[0] * row_ref.shape[1] if len(row_ref.shape) == 3 else row_ref.shape[0]
        all_ref[pl.ds(start, count), :] = row_ref[...].reshape(count, row_ref.shape[-1])
        start += count
    out_ref[...] = tn_dot(placed_ref[...], all_ref[...]).astype(out_ref.dtype)


def per_device(tokens, expert_ids, combine_weight, gate_weight, up_weight, down_weight):
    dest_count = lax.axis_size("expert")
    tensor_count = lax.axis_size("tensor")
    tok_count, width = tokens.shape
    local_count, hidden_part, model = gate_weight.shape
    spread = min(6, dest_count // 2)
    capacity = min(tok_count * 3 // 4, 2 * tok_count * spread // dest_count)
    few = dest_count <= 4
    hidden_count = local_count * hidden_part
    gate_rows = gate_weight.reshape(hidden_count, model)
    up_rows = up_weight.reshape(hidden_count, model)
    down_rows = down_weight.reshape(hidden_count, model)
    slot_lanes = lanes(capacity)

    def dests(step):
        return peer(lax.axis_index("expert"), step, dest_count) if few else step

    whole = pl.BlockSpec(memory_space=VMEM)
    picked = pl.pallas_call(
        functools.partial(select_kernel, dest_count, capacity, local_count, dests),
        out_shape=[jax.ShapeDtypeStruct((1, capacity, width), jnp.bfloat16)] * dest_count
        + [jax.ShapeDtypeStruct((1, 8, slot_lanes), jnp.bfloat16)] * dest_count
        + [jax.ShapeDtypeStruct((dest_count * capacity, tok_count), jnp.bfloat16)],
        in_specs=[whole] * 3,
        out_specs=[whole] * (2 * dest_count + 1),
        scratch_shapes=[VMEM((lanes(dest_count), tok_count), jnp.float32)],
        compiler_params=pltpu.CompilerParams(vmem_limit_bytes=8 * MIB),
        cost_estimate=pl.CostEstimate(flops=10**8, bytes_accessed=10**6, transcendentals=0),
        name="select",
    )(expert_ids, combine_weight, tokens)
    row_pieces, share_pieces, placed = list(picked[:dest_count]), list(picked[dest_count:-1]), picked[-1]
    if few:
        for step in range(1, dest_count):
            share_pieces[step] = exchange(share_pieces[step], "expert", step, dest_count)
            row_pieces[step] = exchange(row_pieces[step], "expert", step, dest_count)
    else:
        row_pieces = [lax.all_to_all(jnp.concatenate(row_pieces), "expert", 0, 0, tiled=True)]
        share_pieces = [lax.all_to_all(jnp.concatenate(share_pieces), "expert", 0, 0, tiled=True)]

    def features(step):
        return back(lax.axis_index("tensor"), step, tensor_count)

    def run_experts(rows, share):
        blocks = rows[0].shape[0]
        by_block = lambda shape: pl.BlockSpec((1,) + shape, lambda block: (block, 0, 0))
        fixed = lambda array: pl.BlockSpec(array.shape, lambda block: (0, 0), pipeline_mode=pl.Buffered(1))
        row_spec = by_block((capacity, width))
        if blocks == 1:
            how = dict(in_specs=[whole] * (tensor_count + 4), out_specs=[whole] * tensor_count)
        else:
            how = dict(
                grid=(blocks,),
                in_specs=[row_spec] * tensor_count
                + [by_block((8, slot_lanes)), fixed(gate_rows), fixed(up_rows), fixed(down_rows)],
                out_specs=[row_spec] * tensor_count,
            )
        return pl.pallas_call(
            functools.partial(expert_kernel, tensor_count, features, hidden_part),
            out_shape=[
                jax.ShapeDtypeStruct((blocks, capacity, width), jnp.float32 if step == 0 else jnp.bfloat16)
                for step in range(tensor_count)
            ],
            scratch_shapes=[VMEM((capacity, model), jnp.bfloat16)],
            compiler_params=pltpu.CompilerParams(vmem_limit_bytes=24 * MIB),
            cost_estimate=pl.CostEstimate(
                flops=6 * blocks * capacity * hidden_count * model,
                bytes_accessed=6 * hidden_count * model,
                transcendentals=blocks * capacity * hidden_count,
            ),
            name="experts",
            **how,
        )(*rows, share, gate_rows, up_rows, down_rows)

    returned = []
    for step, (rows, share) in enumerate(zip(row_pieces, share_pieces)):
        gathered = [rows] + [exchange(rows, "tensor", turn, tensor_count) for turn in range(1, tensor_count)]
        parts = run_experts(gathered, share)
        total = parts[0]
        for turn in range(1, tensor_count):
            total = total + give_back(parts[turn], "tensor", turn, tensor_count).astype(jnp.float32)
        total = total.astype(jnp.bfloat16)
        if few:
            returned.append(give_back(total, "expert", step, dest_count) if step else total)
        else:
            returned.append(lax.all_to_all(total, "expert", 0, 0, tiled=True))
    return pl.pallas_call(
        combine_kernel,
        out_shape=jax.ShapeDtypeStruct((tok_count, width), jnp.bfloat16),
        in_specs=[whole] * (len(returned) + 1),
        out_specs=whole,
        scratch_shapes=[VMEM((dest_count * capacity, width), jnp.bfloat16)],
        compiler_params=pltpu.CompilerParams(vmem_limit_bytes=8 * MIB),
        name="combine",
    )(placed, *returned)


def solution(mesh):
    in_specs = (
        P(("dp", "expert"), "tensor"),
        P(("dp", "expert"), None),
        P(("dp", "expert"), None),
        P("expert", "tensor", None),
        P("expert", "tensor", None),
        P("expert", "tensor", None),
    )
    out_specs = P(("dp", "expert"), "tensor")
    return jax.shard_map(
        per_device, mesh=mesh, in_specs=in_specs, out_specs=out_specs, check_vma=False
    )
```
